32 devices in a mesh: gx: 4 (over y, x), gy: 2 (over core), gz: 4 (over z).
Axes of the slice: x: 2, y: 2, z: 4, core: 2. Of those that a mesh axis runs over, the one named last changes fastest.
Arguments:
- gradient: bfloat16 [32, 32, 16, 512], P(None, 'gx', 'gy', 'gz'), may hold values from -6 to 6
- noise_draw: bfloat16 [32, 32, 16, 512], P(None, 'gx', 'gy', 'gz'), may hold values from -6 to 6
- current: float32 [32, 32, 16, 512], P(None, 'gx', 'gy', 'gz'), may hold values from -6 to 6
- eigvectors: bfloat16 [32, 16, 512, 512], P('gx', 'gy', 'gz'), may hold values from -0.125 to 0.125
- eigvalues: float32 [512], replicated, may hold values from 0.05 to 50
- reaction: float32 [32, 16, 512], P('gx', 'gy', 'gz'), may hold values from 0.25 to 4
Outputs:
- proposal: float32 [32, 32, 16, 512], P(None, 'gx', 'gy', 'gz')
The draws below stay inside these ranges and needn't reach their ends.
All inputs are finite; a program needn't handle non-finite values.
Results may differ from the reference program's by a relative error of at most 0.00031.
Values sent between devices are 32-bit elements; how exact they have to be, the bound alone decides.
A program may use at most 64 MiB of HBM per device.

```python
import math
import jax
import jax.numpy as jnp
from jax import lax

R = 512
CHAINS = 32
SWEEPS = 4
NX = 32
NY = 16
NZ = 512


def block_scale(stream_key, dims, cuts, least, largest):
    loudness, own = 1.0, jax.random.fold_in(stream_key, 6)
    for dim, parts in cuts:
        heights = jnp.exp(jax.random.uniform(jax.random.fold_in(own, dim), (parts,), jnp.float32, least / len(cuts), largest / len(cuts)))
        loudness = loudness * jnp.repeat(heights, dims[dim] // parts).reshape([-1 if axis == dim else 1 for axis in range(len(dims))])
    return loudness


def normal_values(rng, shape, spread, reach, cuts=(), kind=jnp.bfloat16):
    entries = jax.random.normal(rng, shape, jnp.float32) * spread
    if len(cuts) > 0:
        entries = block_scale(rng, shape, cuts, -0.22, 0.18) * entries
    return jnp.clip(entries, min=-reach, max=reach).astype(kind)


def setup_inputs(seed: int = 0) -> dict:
    streams_of = jax.random.split(jax.random.key(seed), 7)
    gradient = normal_values(streams_of[0], (CHAINS, NX, NY, NZ), 1.0, 6.0, ((1, 4), (2, 2), (3, 4)))
    noise_draw = normal_values(streams_of[1], (CHAINS, NX, NY, NZ), 1.0, 6.0, ((1, 4), (2, 2), (3, 4)))
    current = normal_values(streams_of[2], (CHAINS, NX, NY, NZ), 1.0, 6.0, ((1, 4), (2, 2), (3, 4)), jnp.float32)
    eigvectors = normal_values(streams_of[3], (NX, NY, NZ, R), ((R * NX * NY * NZ) ** -0.25), 0.125, ((0, 4), (1, 2), (2, 4)))
    eigvalues = jnp.clip(jnp.exp(jax.random.uniform(streams_of[4], (R,), jnp.float32, math.log(0.05), math.log(50.0))), 0.05, 50.0)
    reaction = jnp.clip(jnp.exp(math.log(4.0) - 2.7725887 * jax.random.uniform(streams_of[5], (NX, NY, NZ), jnp.float32) ** block_scale(streams_of[5], (NX, NY, NZ), ((0, 4), (1, 2), (2, 4)), -0.2, 0.2)), 0.25, 4.0)
    return dict(gradient=gradient, noise_draw=noise_draw, current=current, eigvectors=eigvectors, eigvalues=eigvalues, reaction=reaction)


def neighbours(field):
    padded = jnp.pad(field, ((0, 0), (1, 1), (1, 1), (1, 1)))
    total = padded[:, 2:, 1:-1, 1:-1] + padded[:, :-2, 1:-1, 1:-1]
    total = total + padded[:, 1:-1, 2:, 1:-1] + padded[:, 1:-1, :-2, 1:-1]
    total = total + padded[:, 1:-1, 1:-1, 2:] + padded[:, 1:-1, 1:-1, :-2]
    return total

def reference(gradient, noise_draw, current, eigvectors, eigvalues, reaction):
    stacked = jnp.concatenate([gradient, noise_draw], 0)
    slabs = jnp.moveaxis(stacked, 1, 0)

    def accumulate(total, pair):
        basis_slab, data_slab = pair
        rows = basis_slab.reshape(-1, R)
        vectors = data_slab.reshape(data_slab.shape[0], -1)
        return (total + jnp.dot(vectors, rows, preferred_element_type=jnp.float32), None)
    start = jnp.zeros((2 * CHAINS, R), jnp.float32)
    sums, _ = lax.scan(accumulate, start, (eigvectors, slabs))
    proj_grad = sums[:CHAINS]
    proj_noise = sums[CHAINS:]
    damp = eigvalues / (eigvalues + 1.0)
    root_damp = 1.0 - 1.0 / jnp.sqrt(1.0 + eigvalues)
    coef = (0.5 * damp * proj_grad - 1.0 * root_damp * proj_noise).astype(jnp.bfloat16)

    def expand(basis_slab):
        rows = basis_slab.reshape(-1, R)
        return lax.dot_general(coef, rows, (((1,), (1,)), ((), ())), preferred_element_type=jnp.float32)
    corr_slabs = lax.map(expand, eigvectors)
    corr = jnp.moveaxis(corr_slabs, 0, 1).reshape(current.shape)
    source = -0.5 * gradient.astype(jnp.float32) + 1.0 * noise_draw.astype(jnp.float32) + corr
    diagonal = reaction + 6.0
    field = source / diagonal
    for sweep_index in range(SWEEPS - 1):
        field = (source + neighbours(field)) / diagonal
    return current + field
```

```python
import functools

import jax
import jax.numpy as jnp
from jax import lax
from jax.experimental import pallas as pl
from jax.experimental.pallas import tpu as pltpu
from jax.sharding import PartitionSpec as P

SWEEPS = 4
GROUPS = 4
LEFT = 65536
RELAYED = ((2, 3), (2, 3), ())
ORDER = (
    ("F2", "F3", "E0", "E1", "I0", "I1", "E2", "I2", "E3", "I3"),
    ("F2", "F3", "I0", "E0", "I1", "E1", "I2", "E2", "I3", "E3"),
    ("F2", "F3", "I0", "E0", "I1", "E1", "I2", "E2", "I3", "E3"),
)
MESH = pl.DeviceIdType.MESH
AXES = ("gx", "gy", "gz")


def pitch_of(rows):
    return rows + 8 if (rows // 8) % 2 == 0 else rows


def kernel(
    sizes, shape, g_h, n_h, cur_h, eig_h, ev_ref, rea_h, out_v,
    eig_v, gb, nb, gf, nf, cur_v, rdv, src, fields, zout, zin, relay,
    part, got1, got2, full, load_sem,
    send1, recv1, send2, recv2, send3, recv3, hsend, hrecv, rsend, rrecv,
):
    C, X, Y, Z, R = shape
    NX, NY, NZ = sizes
    G = src.shape[0]
    CG = C // G
    XY = X * Y
    PT = pitch_of(XY)
    S = SWEEPS - 1
    PL = NX * NY
    rows = part.shape[1]
    pos = {a: lax.axis_index(a) for a in AXES}
    count = dict(zip(AXES, sizes))
    me_p = pos["gx"] * NY + pos["gy"]
    me_z = pos["gz"]

    loads = [
        pltpu.make_async_copy(g_h, gb, load_sem.at[0]),
        pltpu.make_async_copy(n_h, nb, load_sem.at[1]),
        pltpu.make_async_copy(rea_h, rdv, load_sem.at[2]),
    ]
    eig_loads = [
        pltpu.make_async_copy(eig_h.at[x], eig_v.at[x], load_sem.at[4 + x]) for x in range(X)
    ]
    for c in loads + eig_loads:
        c.start()

    @pl.loop(0, C)
    def _(c):
        a = pl.ds(pl.multiple_of(c * XY, 8), XY)
        b = pl.ds(pl.multiple_of(c * PT, 8), XY)
        pltpu.make_async_copy(cur_h.at[a], cur_v.at[b], load_sem.at[3]).start()

    barrier = pltpu.get_barrier_semaphore()

    def plane_peer(d):
        q = lax.rem(me_p + d, PL)
        return {"gx": q // NY, "gy": lax.rem(q, NY)}, q

    for d in range(1, PL):
        pl.semaphore_signal(barrier, inc=1, device_id=plane_peer(d)[0], device_id_type=MESH)
    for d in range(1, NZ):
        pl.semaphore_signal(
            barrier, inc=1, device_id={"gz": lax.rem(me_z + d, NZ)}, device_id_type=MESH
        )

    zeros = jnp.zeros((Y, CG, Z), jnp.float32)
    zerosy = jnp.zeros((X, CG, Z), jnp.float32)

    def fill(cond, fn):
        if cond is True:
            fn()
        else:
            pl.when(cond)(fn)

    def low_edge(a):
        return True if count[a] == 1 else pos[a] == 0

    def high_edge(a):
        return True if count[a] == 1 else pos[a] == count[a] - 1

    def fills():
        def x0():
            for k in range(S):
                for g in range(G):
                    fields[k, g, 0, 1 : Y + 1] = zeros
        def x1():
            for k in range(S):
                for g in range(G):
                    fields[k, g, X + 1, 1 : Y + 1] = zeros
        def y0():
            for k in range(S):
                for g in range(G):
                    fields[k, g, 1 : X + 1, 0] = zerosy
        def y1():
            for k in range(S):
                for g in range(G):
                    fields[k, g, 1 : X + 1, Y + 1] = zerosy
        def z0():
            for k in range(S):
                for g in range(G):
                    zin[k, g, 0] = jnp.zeros((CG, Z), jnp.float32)
        def z1():
            for k in range(S):
                for g in range(G):
                    zin[k, g, 1] = jnp.zeros((CG, Z), jnp.float32)
        fill(low_edge("gx"), x0)
        fill(high_edge("gx"), x1)
        fill(low_edge("gy"), y0)
        fill(high_edge("gy"), y1)
        fill(low_edge("gz"), z0)
        fill(high_edge("gz"), z1)

    loads[0].wait()
    loads[1].wait()

    @pl.loop(0, C)
    def _(c):
        a = pl.ds(pl.multiple_of(c * XY, 8), XY)
        b = pl.ds(pl.multiple_of(c * PT, 8), XY)
        gf[b, :] = gb[a, :].astype(jnp.float32)
        nf[b, :] = nb[a, :].astype(jnp.float32)

    acc = None
    for x in range(X):
        cols = []
        for y in range(Y):
            at = pl.ds(x * Y + y, C, stride=PT)
            cols.append(jnp.concatenate([gf[at, :], nf[at, :]], 0).astype(jnp.bfloat16))
        lhs = jnp.concatenate(cols, 1)
        eig_loads[x].wait()
        term = jnp.dot(lhs, eig_v[x], preferred_element_type=jnp.float32)
        acc = term if acc is None else acc + term
    ev = ev_ref[...]
    damp = ev / (ev + 1.0)
    root_damp = 1.0 - 1.0 / jnp.sqrt(1.0 + ev)
    comb = (0.5 * damp) * acc[:C] - root_damp * acc[C:]
    RT = R // 128
    tiles = [(c, r) for c in range(C // 8) for r in range(RT)]
    for t, (c, r) in enumerate(tiles):
        tile = comb[c * 8 : (c + 1) * 8, r * 128 : (r + 1) * 128]
        if rows >= 8:
            o = (t * 8) % rows
            part[(t * 8) // rows, o : o + 8, :] = tile
        else:
            for j in range(8 // rows):
                part[(t * 8) // rows + j] = tile[j * rows : (j + 1) * rows]

    pl.semaphore_wait(barrier, PL - 1 + NZ - 1)

    copies1 = []
    for d in range(1, PL):
        dev, q = plane_peer(d)
        copies1.append(pltpu.make_async_remote_copy(
            src_ref=part.at[q], dst_ref=got1.at[d],
            send_sem=send1.at[d], recv_sem=recv1.at[d],
            device_id=dev, device_id_type=MESH))
    for c in copies1:
        c.start()

    fills()
    loads[2].wait()
    rdv[...] = 1.0 / (rdv[...] + 6.0)

    @pl.loop(0, X)
    def _(x):
        for y in range(Y):
            for g in range(G):
                at = pl.ds(g * CG * PT + x * Y + y, CG, stride=PT)
                src[g, x, y] = -0.5 * gf[at, :] + nf[at, :]

    total = part[me_p]
    for d in range(1, PL):
        copies1[d - 1].wait_recv()
        total = total + got1[d]
    got2[me_z] = total
    copies2 = []
    for d in range(1, NZ):
        copies2.append(pltpu.make_async_remote_copy(
            src_ref=got2.at[me_z], dst_ref=got2.at[me_z],
            send_sem=send2.at[d], recv_sem=recv2.at[d],
            device_id={"gz": lax.rem(me_z + d, NZ)}, device_id_type=MESH))
    for c in copies2:
        c.start()
    for c in copies2:
        c.wait_recv()
    total = got2[0]
    for j in range(1, NZ):
        total = total + got2[j]
    full[me_p] = total
    copies3 = []
    for d in range(1, PL):
        copies3.append(pltpu.make_async_remote_copy(
            src_ref=full.at[me_p], dst_ref=full.at[me_p],
            send_sem=send3.at[d], recv_sem=recv3.at[d],
            device_id=plane_peer(d)[0], device_id_type=MESH))
    for c in copies3:
        c.start()
    for c in copies3:
        c.wait_recv()
    bands = []
    for c in range(C // 8):
        band = []
        for r in range(RT):
            t = c * RT + r
            if rows >= 8:
                o = (t * 8) % rows
                band.append(full[(t * 8) // rows, o : o + 8, :])
            else:
                band.append(jnp.concatenate(
                    [full[(t * 8) // rows + j] for j in range(8 // rows)], 0))
        bands.append(jnp.concatenate(band, 1))
    coef = jnp.concatenate(bands, 0).astype(jnp.bfloat16)

    lane = lax.broadcasted_iota(jnp.int32, (CG, Z), 1)
    pair = lane // 2
    odd = lax.rem(lane, 2) == 1
    at_low = lane == 0
    at_high = lane == Z - 1

    via = count["gx"] == 4

    def relayed(k, g):
        return via and g in RELAYED[k]

    def halo(k, g, axis, sign):
        i = AXES.index(axis) * 2 + (sign > 0)
        n = count[axis]
        recv = hrecv.at[k, g, i]
        to = lax.rem(pos[axis] + (sign + n), n)
        if axis == "gx":
            s = fields.at[k, g, X if sign > 0 else 1, 1 : Y + 1]
            d = fields.at[k, g, 0 if sign > 0 else X + 1, 1 : Y + 1]
        elif axis == "gy":
            s = fields.at[k, g, 1 : X + 1, Y if sign > 0 else 1]
            d = fields.at[k, g, 1 : X + 1, 0 if sign > 0 else Y + 1]
        else:
            s = zout.at[k, g]
            d = zin.at[k, g, 0 if sign > 0 else 1]
        copy = pltpu.make_async_remote_copy(
            src_ref=s, dst_ref=d, send_sem=hsend.at[k, g, i], recv_sem=recv,
            device_id={axis: to}, device_id_type=MESH)
        up, down = pos[axis] < n - 1, pos[axis] > 0
        return copy, (up if sign > 0 else down), (down if sign > 0 else up)

    def hop(k, g, sign):
        i = 1 if sign > 0 else 0
        copy = pltpu.make_async_remote_copy(
            src_ref=fields.at[k, g, X if sign > 0 else 1, 1 : Y + 1], dst_ref=relay.at[k, g],
            send_sem=hsend.at[k, g, i], recv_sem=rrecv.at[k, g],
            device_id={"gx": 3 if sign > 0 else 0}, device_id_type=MESH)
        return copy

    def forward(k, g, sign):
        i = 1 if sign > 0 else 0
        copy = pltpu.make_async_remote_copy(
            src_ref=relay.at[k, g],
            dst_ref=fields.at[k, g, 0 if sign > 0 else X + 1, 1 : Y + 1],
            send_sem=rsend.at[k, g], recv_sem=hrecv.at[k, g, i],
            device_id={"gx": 2 if sign > 0 else 1}, device_id_type=MESH)
        return copy

    ways = [(a, s) for a in AXES if count[a] > 1 for s in (-1, 1)]

    def inner(sign):
        return pos["gx"] == (1 if sign > 0 else 2)

    def send(k, g, axes):
        for a, s in ways:
            if a in axes:
                copy, out, _ = halo(k, g, a, s)
                if a == "gx" and relayed(k, g):
                    pl.when(inner(s))(hop(k, g, s).start)
                    out = out & jnp.logical_not(inner(s))
                pl.when(out)(copy.start)

    def wait_halos(k, g, axes):
        for a, s in ways:
            if a in axes:
                copy, _, come = halo(k, g, a, s)
                pl.when(come)(copy.wait_recv)

    def forwards(k, g, done):
        if relayed(k, g):
            for s, at in ((1, 3), (-1, 0)):
                @pl.when(pos["gx"] == at)
                def _(s=s):
                    if done:
                        forward(k, g, s).wait_send()
                    else:
                        hop(k, g, s).wait_recv()
                        forward(k, g, s).start()

    def wait_sends(k, g):
        for a, s in ways:
            copy, out, _ = halo(k, g, a, s)
            pl.when(out)(copy.wait_send)
        forwards(k, g, True)

    def pack(l, f, old):
        return jnp.where(pair == l, pltpu.roll(f, (2 * l + 1) % Z, 1), old)

    packed = [jnp.zeros((CG, Z), jnp.float32) for _ in range(G)]

    def first(x):
        corr = lax.dot_general(
            coef, eig_v[x], (((1,), (1,)), ((), ())), preferred_element_type=jnp.float32)
        for g in range(G):
            for y in range(Y):
                s = src[g, x, y] + corr[g * CG : (g + 1) * CG, y * Z : (y + 1) * Z]
                src[g, x, y] = s
                f = s * rdv[x, y : y + 1]
                fields[0, g, x + 1, y + 1] = f
                packed[g] = pack(x * Y + y, f, packed[g])

    edges = (0, X - 1) if X > 1 else (0,)
    for x in edges:
        first(x)
    for g in range(G):
        send(0, g, ("gx",))
    for x in range(1, X - 1):
        first(x)
    for g in range(G):
        zout[0, g] = packed[g]
        send(0, g, ("gz", "gy"))

    def step(k, g, x, comb, old):
        for y in range(Y):
            l = x * Y + y
            f = fields[k, g, x + 1, y + 1]
            t = fields[k, g, x + 2, y + 1] + fields[k, g, x, y + 1]
            t = t + (fields[k, g, x + 1, y + 2] + fields[k, g, x + 1, y])
            out = pltpu.roll(comb, (2 * Z - 2 * l - 2) % Z, 1)
            up = jnp.where(at_high, out, pltpu.roll(f, Z - 1, 1))
            down = jnp.where(at_low, out, pltpu.roll(f, 1, 1))
            v = (src[g, x, y] + (t + (up + down))) * rdv[x, y : y + 1]
            if k < S - 1:
                fields[k + 1, g, x + 1, y + 1] = v
                old = pack(l, v, old)
            else:
                at = pl.ds(g * CG * PT + l, CG, stride=PT)
                out_v[at, :] = v + cur_v[at, :]
        return old

    pltpu.make_async_copy(cur_h, cur_v.at[pl.ds(0, C * XY)], load_sem.at[3]).wait()
    zero = jnp.zeros((CG, Z), jnp.float32)
    for k in range(S):
        held, done = {}, []

        def begin(g, k=k, held=held):
            if g not in held:
                wait_halos(k, g, ("gy", "gz"))
                comb = jnp.where(odd, zin[k, g, 1], pltpu.roll(zin[k, g, 0], 2, 1))
                held[g] = [comb, zero]

        for op, g in ((o[0], int(o[1:])) for o in ORDER[k]):
            if op == "F":
                forwards(k, g, False)
                continue
            begin(g)
            if op == "E":
                wait_halos(k, g, ("gx",))
            for x in edges if op == "E" else range(1, X - 1):
                held[g][1] = step(k, g, x, held[g][0], held[g][1])
            done.append(g)
            if k < S - 1:
                if op == "E":
                    send(k + 1, g, ("gx",))
                if done.count(g) == 2:
                    zout[k + 1, g] = held[g][1]
                    send(k + 1, g, ("gy", "gz"))
    for c in copies1 + copies2 + copies3:
        c.wait_send()
    for k in range(S):
        for g in range(G):
            wait_sends(k, g)


def finish(v, out_h, sem):
    C, XY, _ = out_h.shape
    c = pltpu.make_async_copy(v.at[:, pl.ds(0, XY)], out_h, sem)
    c.start()
    c.wait()


def body(sizes, gradient, noise_draw, current, eigvectors, eigvalues, reaction):
    C, X, Y, Z = gradient.shape
    R = eigvectors.shape[3]
    NX, NY, NZ = sizes
    PL = NX * NY
    G = GROUPS
    CG = C // G
    S = SWEEPS - 1
    XY = X * Y
    PT = pitch_of(XY)
    f32, bf16 = jnp.float32, jnp.bfloat16
    rows = C * R // 128 // PL
    any_space = pl.BlockSpec(memory_space=pltpu.HBM)
    vmem = pl.BlockSpec(memory_space=pltpu.VMEM)
    dma = pltpu.SemaphoreType.DMA
    held = pl.pallas_call(
        functools.partial(kernel, sizes, (C, X, Y, Z, R)),
        out_shape=pltpu.VMEM((C * PT, Z), f32),
        in_specs=[any_space] * 4 + [vmem, any_space],
        out_specs=vmem,
        scratch_shapes=[
            pltpu.VMEM((X, Y * Z, R), bf16),
            pltpu.VMEM((C * XY, Z), bf16),
            pltpu.VMEM((C * XY, Z), bf16),
            pltpu.VMEM((C * PT, Z), f32),
            pltpu.VMEM((C * PT, Z), f32),
            pltpu.VMEM((C * PT, Z), f32),
            pltpu.VMEM((X, Y, Z), f32),
            pltpu.VMEM((G, X, Y, CG, Z), f32),
            pltpu.VMEM((S, G, X + 2, Y + 2, CG, Z), f32),
            pltpu.VMEM((S, G, CG, Z), f32),
            pltpu.VMEM((S, G, 2, CG, Z), f32),
            pltpu.VMEM((S, G, Y, CG, Z), f32),
            pltpu.VMEM((PL, rows, 128), f32),
            pltpu.VMEM((PL, rows, 128), f32),
            pltpu.VMEM((NZ, rows, 128), f32),
            pltpu.VMEM((PL, rows, 128), f32),
            dma((4 + X,)),
            dma((PL,)), dma((PL,)),
            dma((NZ,)), dma((NZ,)),
            dma((PL,)), dma((PL,)),
            dma((S, G, 6)), dma((S, G, 6)),
            dma((S, G)), dma((S, G)),
        ],
        compiler_params=pltpu.CompilerParams(
            collective_id=0, has_side_effects=True, vmem_limit_bytes=67043328 - C * PT * Z * 4 - LEFT
        ),
    )(
        gradient.reshape(C * XY, Z),
        noise_draw.reshape(C * XY, Z),
        current.reshape(C * XY, Z),
        eigvectors.reshape(X, Y * Z, R),
        eigvalues.reshape(1, R),
        reaction,
    )
    out = pl.pallas_call(
        finish,
        out_shape=jax.ShapeDtypeStruct((C, XY, Z), f32),
        in_specs=[vmem],
        out_specs=any_space,
        scratch_shapes=[dma],
        compiler_params=pltpu.CompilerParams(vmem_limit_bytes=4 * 1024 * 1024),
    )(held.reshape(C, PT, Z))
    return out.reshape(current.shape)


def solution(mesh):
    return jax.shard_map(
        functools.partial(body, tuple(mesh.shape[a] for a in AXES)),
        mesh=mesh,
        in_specs=(
            P(None, "gx", "gy", "gz"),
            P(None, "gx", "gy", "gz"),
            P(None, "gx", "gy", "gz"),
            P("gx", "gy", "gz", None),
            P(),
            P("gx", "gy", "gz"),
        ),
        out_specs=P(None, "gx", "gy", "gz"),
        check_vma=False,
    )
```

```python
import functools

import jax
import jax.numpy as jnp
from jax import lax
from jax.experimental import pallas as pl
from jax.experimental.pallas import tpu as pltpu
from jax.sharding import PartitionSpec as P

SWEEPS = 4
GROUPS = 4
HALVES = 2
LEFT = 65536
RELAYED = ((2, 3), (3,), ())
ORDER = (("F2", "F3", "E0", "E1", "I0", "I1", "E2", "I2", "E3", "I3"), ("F3", "I0", "E0", "I1", "E1", "I2", "E2", "I3", "E3"), ("F2", "F3", "I0", "E0", "I1", "E1", "I2", "E2", "I3", "E3"))
MESH = pl.DeviceIdType.MESH
AXES = ("gx", "gy", "gz")


def pitch_of(rows):
    return rows + 8 if (rows // 8) % 2 == 0 else rows


def kernel(
    sizes, shape, g_h, n_h, cur_h, eig_h, ev_h, rea_h, out_v,
    eig_v, gb, nb, gf, nf, cur_v, ev_v, rdv, src, fields, zout, zin, relay,
    part, got1, got2, full, load_sem,
    send_sem, recv1, recv2, recv3, hsend, xrecv, yzrecv, rsend, rrecv,
):
    C, X, Y, Z, R = shape
    NX, NY, NZ = sizes
    G = src.shape[0]
    CG = C // G
    XY = X * Y
    PT = pitch_of(XY)
    S = SWEEPS - 1
    PL = NX * NY
    rows = part.shape[1]
    pos = {a: lax.axis_index(a) for a in AXES}
    count = dict(zip(AXES, sizes))
    me_p = pos["gx"] * NY + pos["gy"]
    me_z = pos["gz"]

    loads = [
        pltpu.make_async_copy(g_h, gb, load_sem.at[0]),
        pltpu.make_async_copy(n_h, nb, load_sem.at[1]),
        pltpu.make_async_copy(rea_h, rdv, load_sem.at[2]),
        pltpu.make_async_copy(ev_h, ev_v, load_sem.at[4]),
    ]
    eig_loads = [
        pltpu.make_async_copy(eig_h.at[x], eig_v.at[x], load_sem.at[5 + x]) for x in range(X)
    ]
    for c in loads[:2] + eig_loads + loads[2:]:
        c.start()

    barrier = pltpu.get_barrier_semaphore()

    def plane_peer(d):
        q = lax.rem(me_p + d, PL)
        return {"gx": q // NY, "gy": lax.rem(q, NY)}, q

    for d in range(1, PL):
        pl.semaphore_signal(barrier, inc=1, device_id=plane_peer(d)[0], device_id_type=MESH)
    for d in range(1, NZ):
        pl.semaphore_signal(
            barrier, inc=1, device_id={"gz": lax.rem(me_z + d, NZ)}, device_id_type=MESH
        )

    zeros = jnp.zeros((Y, CG, Z), jnp.float32)
    zerosy = jnp.zeros((X, CG, Z), jnp.float32)

    def fill(cond, fn):
        if cond is True:
            fn()
        else:
            pl.when(cond)(fn)

    def low_edge(a):
        return True if count[a] == 1 else pos[a] == 0

    def high_edge(a):
        return True if count[a] == 1 else pos[a] == count[a] - 1

    def fills():
        def x0():
            for k in range(S):
                for g in range(G):
                    fields[k, g, 0, 1 : Y + 1] = zeros
        def x1():
            for k in range(S):
                for g in range(G):
                    fields[k, g, X + 1, 1 : Y + 1] = zeros
        def y0():
            for k in range(S):
                for g in range(G):
                    fields[k, g, 1 : X + 1, 0] = zerosy
        def y1():
            for k in range(S):
                for g in range(G):
                    fields[k, g, 1 : X + 1, Y + 1] = zerosy
        def z0():
            for k in range(S):
                for g in range(G):
                    zin[k, g, 0] = jnp.zeros((CG, Z), jnp.float32)
        def z1():
            for k in range(S):
                for g in range(G):
                    zin[k, g, 1] = jnp.zeros((CG, Z), jnp.float32)
        fill(low_edge("gx"), x0)
        fill(high_edge("gx"), x1)
        fill(low_edge("gy"), y0)
        fill(high_edge("gy"), y1)
        fill(low_edge("gz"), z0)
        fill(high_edge("gz"), z1)

    loads[0].wait()
    loads[1].wait()

    @pl.loop(0, C)
    def _(c):
        a = pl.ds(pl.multiple_of(c * XY, 8), XY)
        b = pl.ds(pl.multiple_of(c * PT, 8), XY)
        gf[b, :] = gb[a, :].astype(jnp.float32)
        nf[b, :] = nb[a, :].astype(jnp.float32)

    acc = None
    for x in range(X):
        cols = []
        for y in range(Y):
            at = pl.ds(x * Y + y, C, stride=PT)
            cols.append(jnp.concatenate([gf[at, :], nf[at, :]], 0).astype(jnp.bfloat16))
        lhs = jnp.concatenate(cols, 1)
        eig_loads[x].wait()
        term = jnp.dot(lhs, eig_v[x], preferred_element_type=jnp.float32)
        acc = term if acc is None else acc + term
    loads[3].wait()
    ev = ev_v[...]
    damp = ev / (ev + 1.0)
    root_damp = 1.0 - 1.0 / jnp.sqrt(1.0 + ev)
    comb = (0.5 * damp) * acc[:C] - root_damp * acc[C:]
    RT = R // 128
    tiles = [(c, r) for c in range(C // 8) for r in range(RT)]
    for t, (c, r) in enumerate(tiles):
        tile = comb[c * 8 : (c + 1) * 8, r * 128 : (r + 1) * 128]
        if rows >= 8:
            o = (t * 8) % rows
            part[(t * 8) // rows, o : o + 8, :] = tile
        else:
            for j in range(8 // rows):
                part[(t * 8) // rows + j] = tile[j * rows : (j + 1) * rows]

    pl.semaphore_wait(barrier, PL - 1 + NZ - 1)

    copies1 = []
    for d in range(1, PL):
        dev, q = plane_peer(d)
        copies1.append(pltpu.make_async_remote_copy(
            src_ref=part.at[q], dst_ref=got1.at[d],
            send_sem=send_sem.at[0], recv_sem=recv1.at[d - 1],
            device_id=dev, device_id_type=MESH))
    for c in copies1:
        c.start()

    @pl.loop(0, C)
    def _(c):
        a = pl.ds(pl.multiple_of(c * XY, 8), XY)
        b = pl.ds(pl.multiple_of(c * PT, 8), XY)
        pltpu.make_async_copy(cur_h.at[a], cur_v.at[b], load_sem.at[3]).start()

    fills()
    loads[2].wait()
    rdv[...] = 1.0 / (rdv[...] + 6.0)

    @pl.loop(0, X)
    def _(x):
        for y in range(Y):
            for g in range(G):
                at = pl.ds(g * CG * PT + x * Y + y, CG, stride=PT)
                src[g, x, y] = -0.5 * gf[at, :] + nf[at, :]

    total = part[me_p]
    for d in range(1, PL):
        copies1[d - 1].wait_recv()
        total = total + got1[d]
    got2[me_z] = total
    copies2 = []
    for d in range(1, NZ):
        copies2.append(pltpu.make_async_remote_copy(
            src_ref=got2.at[me_z], dst_ref=got2.at[me_z],
            send_sem=send_sem.at[1], recv_sem=recv2.at[d - 1],
            device_id={"gz": lax.rem(me_z + d, NZ)}, device_id_type=MESH))
    for c in copies2:
        c.start()
    for c in copies2:
        c.wait_recv()
    total = got2[0]
    for j in range(1, NZ):
        total = total + got2[j]
    full[me_p] = total
    copies3 = []
    for d in range(1, PL):
        copies3.append(pltpu.make_async_remote_copy(
            src_ref=full.at[me_p], dst_ref=full.at[me_p],
            send_sem=send_sem.at[2], recv_sem=recv3.at[d - 1],
            device_id=plane_peer(d)[0], device_id_type=MESH))
    for c in copies3:
        c.start()
    for c in copies3:
        c.wait_recv()
    bands = []
    for c in range(C // 8):
        band = []
        for r in range(RT):
            t = c * RT + r
            if rows >= 8:
                o = (t * 8) % rows
                band.append(full[(t * 8) // rows, o : o + 8, :])
            else:
                band.append(jnp.concatenate(
                    [full[(t * 8) // rows + j] for j in range(8 // rows)], 0))
        bands.append(jnp.concatenate(band, 1))
    coef = jnp.concatenate(bands, 0).astype(jnp.bfloat16)

    lane = lax.broadcasted_iota(jnp.int32, (CG, Z), 1)
    pair = lane // 2
    zero = jnp.zeros((CG, Z), jnp.float32)
    odd = lax.rem(lane, 2) == 1
    at_low = lane == 0
    at_high = lane == Z - 1

    via = count["gx"] == 4

    relays = [(k, g) for k in range(S) for g in RELAYED[k]] if via else []
    H = yzrecv.shape[1]
    GH = G // H

    def relayed(k, g):
        return (k, g) in relays

    def halo(k, g, axis, sign):
        i = AXES.index(axis) * 2 + (sign > 0)
        n = count[axis]
        recv = xrecv.at[k, g, i] if axis == "gx" else yzrecv.at[k, g // GH, i - 2]
        to = lax.rem(pos[axis] + (sign + n), n)
        if axis == "gx":
            s = fields.at[k, g, X if sign > 0 else 1, 1 : Y + 1]
            d = fields.at[k, g, 0 if sign > 0 else X + 1, 1 : Y + 1]
        elif axis == "gy":
            s = fields.at[k, g, 1 : X + 1, Y if sign > 0 else 1]
            d = fields.at[k, g, 1 : X + 1, 0 if sign > 0 else Y + 1]
        else:
            s = zout.at[k, g]
            d = zin.at[k, g, 0 if sign > 0 else 1]
        copy = pltpu.make_async_remote_copy(
            src_ref=s, dst_ref=d, send_sem=hsend.at[i], recv_sem=recv,
            device_id={axis: to}, device_id_type=MESH)
        up, down = pos[axis] < n - 1, pos[axis] > 0
        return copy, (up if sign > 0 else down), (down if sign > 0 else up)

    def hop(k, g, sign):
        i = 1 if sign > 0 else 0
        copy = pltpu.make_async_remote_copy(
            src_ref=fields.at[k, g, X if sign > 0 else 1, 1 : Y + 1],
            dst_ref=relay.at[relays.index((k, g))],
            send_sem=hsend.at[i], recv_sem=rrecv.at[relays.index((k, g))],
            device_id={"gx": 3 if sign > 0 else 0}, device_id_type=MESH)
        return copy

    def forward(k, g, sign):
        i = 1 if sign > 0 else 0
        copy = pltpu.make_async_remote_copy(
            src_ref=relay.at[relays.index((k, g))],
            dst_ref=fields.at[k, g, 0 if sign > 0 else X + 1, 1 : Y + 1],
            send_sem=rsend.at[0], recv_sem=xrecv.at[k, g, i],
            device_id={"gx": 2 if sign > 0 else 1}, device_id_type=MESH)
        return copy

    ways = [(a, s) for a in AXES if count[a] > 1 for s in (-1, 1)]

    def inner(sign):
        return pos["gx"] == (1 if sign > 0 else 2)

    def send(k, g, axes, signs=(-1, 1)):
        go = []
        for a, s in ways:
            if a in axes and s in signs:
                copy, out, _ = halo(k, g, a, s)
                if a == "gx" and via:
                    go.insert(0, (inner(s), hop(k, g, s) if relayed(k, g) else copy))
                    out = out & jnp.logical_not(inner(s))
                go.append((out, copy))
        for out, copy in go:
            pl.when(out)(copy.start)

    def wait_x(k, g):
        for a, s in ways:
            if a == "gx":
                copy, _, come = halo(k, g, a, s)
                pl.when(come)(copy.wait_recv)

    def wait_yz(k, h):
        r = pl.ds(h * GH, GH)
        for a, s in ways:
            if a == "gx":
                continue
            i = AXES.index(a) * 2 + (s > 0)
            if a == "gy":
                d = fields.at[k, r, 1 : X + 1, 0 if s > 0 else Y + 1]
            else:
                d = zin.at[k, r, 0 if s > 0 else 1]
            come = pos[a] > 0 if s > 0 else pos[a] < count[a] - 1
            pl.when(come)(pltpu.make_async_copy(d, d, yzrecv.at[k, h, i - 2]).wait)

    def forwards(k, g):
        if relayed(k, g):
            for s, at in ((1, 3), (-1, 0)):
                @pl.when(pos["gx"] == at)
                def _(s=s):
                    hop(k, g, s).wait_recv()
                    forward(k, g, s).start()

    def wait_sends():
        for a, s in ways:
            i = AXES.index(a) * 2 + (s > 0)
            if a == "gx":
                d = fields.at[:, :, X if s > 0 else 1, 1 : Y + 1]
            elif a == "gy":
                d = fields.at[:, :, 1 : X + 1, Y if s > 0 else 1]
            else:
                d = zout
            out = pos[a] < count[a] - 1 if s > 0 else pos[a] > 0
            pl.when(out)(pltpu.make_async_copy(d, d, hsend.at[i]).wait)
        if relays:
            @pl.when((pos["gx"] == 0) | (pos["gx"] == 3))
            def _():
                pltpu.make_async_copy(relay, relay, rsend.at[0]).wait()
        for d, i in ((part.at[pl.ds(0, PL - 1)], 0), (got2.at[pl.ds(0, NZ - 1)], 1), (full.at[pl.ds(0, PL - 1)], 2)):
            if d.shape[0]:
                pltpu.make_async_copy(d, d, send_sem.at[i]).wait()

    def pack(k, g):
        out = zero
        for x in range(X):
            for y in range(Y):
                l = x * Y + y
                f = pltpu.roll(fields[k, g, x + 1, y + 1], (2 * l + 1) % Z, 1)
                out = jnp.where(pair == l, f, out)
        zout[k, g] = out

    def first(x):
        corr = lax.dot_general(
            coef, eig_v[x], (((1,), (1,)), ((), ())), preferred_element_type=jnp.float32)
        for g in range(G):
            for y in range(Y):
                s = src[g, x, y] + corr[g * CG : (g + 1) * CG, y * Z : (y + 1) * Z]
                src[g, x, y] = s
                f = s * rdv[x, y : y + 1]
                fields[0, g, x + 1, y + 1] = f

    edges = (0, X - 1) if X > 1 else (0,)
    for x in edges:
        first(x)
        for g in range(G):
            send(0, g, ("gx",), (-1 if x == 0 else 1,) if X > 1 else (-1, 1))
    for x in range(1, X - 1):
        first(x)
    for g in range(G):
        send(0, g, ("gy",))
    for g in range(G):
        pack(0, g)
        send(0, g, ("gz",))

    def step(k, g, x, comb):
        for y in range(Y):
            l = x * Y + y
            f = fields[k, g, x + 1, y + 1]
            t = fields[k, g, x + 2, y + 1] + fields[k, g, x, y + 1]
            t = t + (fields[k, g, x + 1, y + 2] + fields[k, g, x + 1, y])
            out = pltpu.roll(comb, (2 * Z - 2 * l - 2) % Z, 1)
            up = jnp.where(at_high, out, pltpu.roll(f, Z - 1, 1))
            down = jnp.where(at_low, out, pltpu.roll(f, 1, 1))
            v = (src[g, x, y] + (t + (up + down))) * rdv[x, y : y + 1]
            if k < S - 1:
                fields[k + 1, g, x + 1, y + 1] = v
            else:
                at = pl.ds(g * CG * PT + l, CG, stride=PT)
                out_v[at, :] = v + cur_v[at, :]

    pltpu.make_async_copy(cur_h, cur_v.at[pl.ds(0, C * XY)], load_sem.at[3]).wait()
    for k in range(S):
        held, done, ready = {}, [], []

        def begin(g, k=k, held=held, ready=ready):
            if g not in held:
                if g // GH not in ready:
                    ready.append(g // GH)
                    wait_yz(k, g // GH)
                comb = jnp.where(odd, zin[k, g, 1], pltpu.roll(zin[k, g, 0], 2, 1))
                held[g] = comb

        for op, g in ((o[0], int(o[1:])) for o in ORDER[k]):
            if op == "F":
                forwards(k, g)
                continue
            begin(g)
            if op == "E":
                wait_x(k, g)
            for x in edges if op == "E" else range(1, X - 1):
                step(k, g, x, held[g])
            done.append(g)
            if k < S - 1:
                if op == "E":
                    send(k + 1, g, ("gx",))
                if done.count(g) == 2:
                    send(k + 1, g, ("gy",))
                    pack(k + 1, g)
                    send(k + 1, g, ("gz",))
    wait_sends()


def finish(v, out_h, sem):
    C, XY, _ = out_h.shape
    c = pltpu.make_async_copy(v.at[:, pl.ds(0, XY)], out_h, sem)
    c.start()
    c.wait()


def body(sizes, gradient, noise_draw, current, eigvectors, eigvalues, reaction):
    C, X, Y, Z = gradient.shape
    R = eigvectors.shape[3]
    NX, NY, NZ = sizes
    PL = NX * NY
    G = GROUPS
    CG = C // G
    S = SWEEPS - 1
    XY = X * Y
    PT = pitch_of(XY)
    f32, bf16 = jnp.float32, jnp.bfloat16
    rows = C * R // 128 // PL
    NR = max(sum(len(r) for r in RELAYED), 1)
    any_space = pl.BlockSpec(memory_space=pltpu.HBM)
    vmem = pl.BlockSpec(memory_space=pltpu.VMEM)
    dma = pltpu.SemaphoreType.DMA
    held = pl.pallas_call(
        functools.partial(kernel, sizes, (C, X, Y, Z, R)),
        out_shape=pltpu.VMEM((C * PT, Z), f32),
        in_specs=[any_space] * 6,
        out_specs=vmem,
        scratch_shapes=[
            pltpu.VMEM((X, Y * Z, R), bf16),
            pltpu.VMEM((C * XY, Z), bf16),
            pltpu.VMEM((C * XY, Z), bf16),
            pltpu.VMEM((C * PT, Z), f32),
            pltpu.VMEM((C * PT, Z), f32),
            pltpu.VMEM((C * PT, Z), f32),
            pltpu.VMEM((1, R), f32),
            pltpu.VMEM((X, Y, Z), f32),
            pltpu.VMEM((G, X, Y, CG, Z), f32),
            pltpu.VMEM((S, G, X + 2, Y + 2, CG, Z), f32),
            pltpu.VMEM((S, G, CG, Z), f32),
            pltpu.VMEM((S, G, 2, CG, Z), f32),
            pltpu.VMEM((NR, Y, CG, Z), f32),
            pltpu.VMEM((PL, rows, 128), f32),
            pltpu.VMEM((PL, rows, 128), f32),
            pltpu.VMEM((NZ, rows, 128), f32),
            pltpu.VMEM((PL, rows, 128), f32),
            dma((5 + X,)),
            dma((3,)),
            dma((max(PL - 1, 1),)), dma((max(NZ - 1, 1),)), dma((max(PL - 1, 1),)),
            dma((6,)), dma((S, G, 2)), dma((S, HALVES, 4)),
            dma((1,)), dma((NR,)),
        ],
        compiler_params=pltpu.CompilerParams(
            collective_id=0, has_side_effects=True, vmem_limit_bytes=67043328 - C * PT * Z * 4 - LEFT
        ),
    )(
        gradient.reshape(C * XY, Z),
        noise_draw.reshape(C * XY, Z),
        current.reshape(C * XY, Z),
        eigvectors.reshape(X, Y * Z, R),
        eigvalues.reshape(1, R),
        reaction,
    )
    out = pl.pallas_call(
        finish,
        out_shape=jax.ShapeDtypeStruct((C, XY, Z), f32),
        in_specs=[vmem],
        out_specs=any_space,
        scratch_shapes=[dma],
        compiler_params=pltpu.CompilerParams(vmem_limit_bytes=4 * 1024 * 1024),
    )(held.reshape(C, PT, Z))
    return out.reshape(current.shape)


def solution(mesh):
    return jax.shard_map(
        functools.partial(body, tuple(mesh.shape[a] for a in AXES)),
        mesh=mesh,
        in_specs=(
            P(None, "gx", "gy", "gz"),
            P(None, "gx", "gy", "gz"),
            P(None, "gx", "gy", "gz"),
            P("gx", "gy", "gz", None),
            P(),
            P("gx", "gy", "gz"),
        ),
        out_specs=P(None, "gx", "gy", "gz"),
        check_vma=False,
    )
```

```python
import functools

import jax
import jax.numpy as jnp
from jax import lax
from jax.experimental import pallas as pl
from jax.experimental.pallas import tpu as pltpu
from jax.sharding import PartitionSpec as P

SWEEPS = 4
GROUPS = 4
HALVES = 2
FLIGHT = 8
LEFT = 65536
RELAYED = ((2, 3), (0,), (0,))
ORDER = (("F2", "F3", "E0", "E1", "I0", "I1", "E2", "E3", "I2", "I3"), ("F0", "I0", "E0", "I1", "E1", "I2", "E2", "I3", "E3"), ("F0", "I0", "E0", "I1", "E1", "I2", "E2", "I3", "E3"))
MESH = pl.DeviceIdType.MESH
AXES = ("gx", "gy", "gz")


def pitch_of(rows):
    return rows + 8 if (rows // 8) % 2 == 0 else rows


def kernel(
    sizes, shape, g_h, n_h, cur_h, eig_h, ev_h, rea_h, out_v,
    eig_v, gb, nb, gf, nf, cur_v, ev_v, rdv, src, fields, zout, zin, zout_e, zin_e, relay,
    part, got1, got2, full, load_sem,
    send_sem, recv1, recv2, recv3, hsend, xrecv, yzrecv, early, rsend, rrecv,
):
    C, X, Y, Z, R = shape
    NX, NY, NZ = sizes
    G = src.shape[0]
    CG = C // G
    XY = X * Y
    PT = pitch_of(XY)
    S = SWEEPS - 1
    PL = NX * NY
    rows = part.shape[1]
    pos = {a: lax.axis_index(a) for a in AXES}
    count = dict(zip(AXES, sizes))
    me_p = pos["gx"] * NY + pos["gy"]
    OW = 2 if NY % 2 == 0 else 1
    NO = PL // OW

    def owns(q):
        return True if OW == 1 else lax.rem(q, OW) == OW - 1

    mine = owns(me_p)
    me_o = me_p // OW
    me_z = pos["gz"]

    loads = [
        pltpu.make_async_copy(g_h, gb, load_sem.at[0]),
        pltpu.make_async_copy(n_h, nb, load_sem.at[1]),
        pltpu.make_async_copy(rea_h, rdv, load_sem.at[2]),
        pltpu.make_async_copy(ev_h, ev_v, load_sem.at[4]),
    ]
    eig_loads = [
        pltpu.make_async_copy(eig_h.at[x], eig_v.at[x], load_sem.at[5 + x]) for x in range(X)
    ]
    for c in loads[:2] + eig_loads[:FLIGHT]:
        c.start()

    barrier = pltpu.get_barrier_semaphore()

    def plane_peer(d):
        q = lax.rem(me_p + d, PL)
        return {"gx": q // NY, "gy": lax.rem(q, NY)}, q

    for d in range(1, PL):
        pl.semaphore_signal(barrier, inc=1, device_id=plane_peer(d)[0], device_id_type=MESH)
    for d in range(1, NZ):
        pl.semaphore_signal(
            barrier, inc=1, device_id={"gz": lax.rem(me_z + d, NZ)}, device_id_type=MESH
        )

    zeros = jnp.zeros((Y, CG, Z), jnp.float32)
    zerosy = jnp.zeros((X, CG, Z), jnp.float32)

    def fill(cond, fn):
        if cond is True:
            fn()
        else:
            pl.when(cond)(fn)

    when = fill

    def low_edge(a):
        return True if count[a] == 1 else pos[a] == 0

    def high_edge(a):
        return True if count[a] == 1 else pos[a] == count[a] - 1

    def fills():
        def x0():
            for k in range(S):
                for g in range(G):
                    fields[k, g, 0, 1 : Y + 1] = zeros
        def x1():
            for k in range(S):
                for g in range(G):
                    fields[k, g, X + 1, 1 : Y + 1] = zeros
        def y0():
            for k in range(S):
                for g in range(G):
                    fields[k, g, 1 : X + 1, 0] = zerosy
        def y1():
            for k in range(S):
                for g in range(G):
                    fields[k, g, 1 : X + 1, Y + 1] = zerosy
        def z0():
            for k in range(S):
                for g in range(G):
                    zin[k, g, 0] = jnp.zeros((CG, Z), jnp.float32)
            zin_e[0] = jnp.zeros((G, CG, Z), jnp.float32)
        def z1():
            for k in range(S):
                for g in range(G):
                    zin[k, g, 1] = jnp.zeros((CG, Z), jnp.float32)
            zin_e[1] = jnp.zeros((G, CG, Z), jnp.float32)
        fill(low_edge("gx"), x0)
        fill(high_edge("gx"), x1)
        fill(low_edge("gy"), y0)
        fill(high_edge("gy"), y1)
        fill(low_edge("gz"), z0)
        fill(high_edge("gz"), z1)

    loads[0].wait()
    loads[1].wait()

    @pl.loop(0, C)
    def _(c):
        a = pl.ds(pl.multiple_of(c * XY, 8), XY)
        b = pl.ds(pl.multiple_of(c * PT, 8), XY)
        gf[b, :] = gb[a, :].astype(jnp.float32)
        nf[b, :] = nb[a, :].astype(jnp.float32)

    acc = None
    for x in range(X):
        cols = []
        for y in range(Y):
            at = pl.ds(x * Y + y, C, stride=PT)
            cols.append(jnp.concatenate([gf[at, :], nf[at, :]], 0).astype(jnp.bfloat16))
        lhs = jnp.concatenate(cols, 1)
        eig_loads[x].wait()
        for c in eig_loads[x + FLIGHT : x + FLIGHT + 1] or (loads[2:] if x == max(X - FLIGHT, 0) else []):
            c.start()
        term = jnp.dot(lhs, eig_v[x], preferred_element_type=jnp.float32)
        acc = term if acc is None else acc + term
    loads[3].wait()
    ev = ev_v[...]
    damp = ev / (ev + 1.0)
    root_damp = 1.0 - 1.0 / jnp.sqrt(1.0 + ev)
    comb = (0.5 * damp) * acc[:C] - root_damp * acc[C:]
    RT = R // 128
    tiles = [(c, r) for c in range(C // 8) for r in range(RT)]
    for t, (c, r) in enumerate(tiles):
        tile = comb[c * 8 : (c + 1) * 8, r * 128 : (r + 1) * 128]
        if rows >= 8:
            o = (t * 8) % rows
            part[(t * 8) // rows, o : o + 8, :] = tile
        else:
            for j in range(8 // rows):
                part[(t * 8) // rows + j] = tile[j * rows : (j + 1) * rows]

    pl.semaphore_wait(barrier, PL - 1 + NZ - 1)

    copies1 = []
    for d in range(1, PL):
        dev, q = plane_peer(d)
        copies1.append(pltpu.make_async_remote_copy(
            src_ref=part.at[q // OW], dst_ref=got1.at[d],
            send_sem=send_sem.at[0], recv_sem=recv1.at[d - 1],
            device_id=dev, device_id_type=MESH))
        when(owns(q), copies1[-1].start)

    @pl.loop(0, C)
    def _(c):
        a = pl.ds(pl.multiple_of(c * XY, 8), XY)
        b = pl.ds(pl.multiple_of(c * PT, 8), XY)
        pltpu.make_async_copy(cur_h.at[a], cur_v.at[b], load_sem.at[3]).start()

    fills()
    loads[2].wait()
    rdv[...] = 1.0 / (rdv[...] + 6.0)

    @pl.loop(0, X)
    def _(x):
        for y in range(Y):
            for g in range(G):
                at = pl.ds(g * CG * PT + x * Y + y, CG, stride=PT)
                src[g, x, y] = -0.5 * gf[at, :] + nf[at, :]

    def reduce1():
        total = part[me_o]
        for d in range(1, PL):
            copies1[d - 1].wait_recv()
            total = total + got1[d]
        got2[me_z] = total
    when(mine, reduce1)
    def reduce2():
        copies = []
        for d in range(1, NZ):
            copies.append(pltpu.make_async_remote_copy(
                src_ref=got2.at[me_z], dst_ref=got2.at[me_z],
                send_sem=send_sem.at[1], recv_sem=recv2.at[d - 1],
                device_id={"gz": lax.rem(me_z + d, NZ)}, device_id_type=MESH))
        for c in copies:
            c.start()
        for c in copies:
            c.wait_recv()
        total = got2[0]
        for j in range(1, NZ):
            total = total + got2[j]
        full[me_o] = total
        for d in range(1, PL):
            pltpu.make_async_remote_copy(
                src_ref=full.at[me_o], dst_ref=full.at[me_o],
                send_sem=send_sem.at[2], recv_sem=recv3.at[d - 1],
                device_id=plane_peer(d)[0], device_id_type=MESH).start()
    when(mine, reduce2)
    for d in range(1, PL):
        q = lax.rem(me_p + (PL - d), PL)
        r = full.at[q // OW]
        when(owns(q), pltpu.make_async_copy(r, r, recv3.at[d - 1]).wait)
    bands = []
    for c in range(C // 8):
        band = []
        for r in range(RT):
            t = c * RT + r
            if rows >= 8:
                o = (t * 8) % rows
                band.append(full[(t * 8) // rows, o : o + 8, :])
            else:
                band.append(jnp.concatenate(
                    [full[(t * 8) // rows + j] for j in range(8 // rows)], 0))
        bands.append(jnp.concatenate(band, 1))
    coef = jnp.concatenate(bands, 0).astype(jnp.bfloat16)

    lane = lax.broadcasted_iota(jnp.int32, (CG, Z), 1)
    pair = lane // 2
    zero = jnp.zeros((CG, Z), jnp.float32)
    odd = lax.rem(lane, 2) == 1
    at_low = lane == 0
    at_high = lane == Z - 1

    via = count["gx"] == 4

    relays = [(k, g) for k in range(S) for g in RELAYED[k]] if via else []
    H = yzrecv.shape[1]
    GH = G // H

    inner_rows = slice(2, X)

    def early_copies(axis, sign):
        n = count[axis]
        dev = {axis: lax.rem(pos[axis] + (sign + n), n)}
        i = AXES.index(axis) * 2 + (sign > 0)
        if axis == "gz":
            pairs = [(zout_e, zin_e.at[0 if sign > 0 else 1])]
            i = 6 + (sign > 0)
        else:
            pairs = [(fields.at[0, :, x, Y if sign > 0 else 1], fields.at[0, :, x, 0 if sign > 0 else Y + 1])
                     for x in (1, X)]
        return [pltpu.make_async_remote_copy(
            src_ref=a, dst_ref=b, send_sem=hsend.at[i],
            recv_sem=early.at[AXES.index(axis) * 2 - 2 + (sign > 0)],
            device_id=dev, device_id_type=MESH) for a, b in pairs]

    def send_early():
        for a, s in ways:
            if a != "gx":
                out = pos[a] < count[a] - 1 if s > 0 else pos[a] > 0
                for c in early_copies(a, s):
                    pl.when(out)(c.start)

    def wait_early():
        for a, s in ways:
            if a != "gx":
                come = pos[a] > 0 if s > 0 else pos[a] < count[a] - 1
                d = zin_e.at[0] if a == "gz" else fields.at[0, :, pl.ds(1, 2), 0]
                i = AXES.index(a) * 2 - 2 + (s > 0)
                pl.when(come)(pltpu.make_async_copy(d, d, early.at[i]).wait)

    def relayed(k, g):
        return (k, g) in relays

    def halo(k, g, axis, sign):
        i = AXES.index(axis) * 2 + (sign > 0)
        n = count[axis]
        recv = xrecv.at[k, g, i] if axis == "gx" else yzrecv.at[k, g // GH, i - 2]
        to = lax.rem(pos[axis] + (sign + n), n)
        if axis == "gx":
            s = fields.at[k, g, X if sign > 0 else 1, 1 : Y + 1]
            d = fields.at[k, g, 0 if sign > 0 else X + 1, 1 : Y + 1]
        elif axis == "gy":
            r = inner_rows if k == 0 else slice(1, X + 1)
            s = fields.at[k, g, r, Y if sign > 0 else 1]
            d = fields.at[k, g, r, 0 if sign > 0 else Y + 1]
        else:
            s = zout.at[k, g]
            d = zin.at[k, g, 0 if sign > 0 else 1]
        copy = pltpu.make_async_remote_copy(
            src_ref=s, dst_ref=d, send_sem=hsend.at[i], recv_sem=recv,
            device_id={axis: to}, device_id_type=MESH)
        up, down = pos[axis] < n - 1, pos[axis] > 0
        return copy, (up if sign > 0 else down), (down if sign > 0 else up)

    def hop(k, g, sign):
        i = 1 if sign > 0 else 0
        copy = pltpu.make_async_remote_copy(
            src_ref=fields.at[k, g, X if sign > 0 else 1, 1 : Y + 1],
            dst_ref=relay.at[relays.index((k, g))],
            send_sem=hsend.at[i], recv_sem=rrecv.at[relays.index((k, g))],
            device_id={"gx": 3 if sign > 0 else 0}, device_id_type=MESH)
        return copy

    def forward(k, g, sign):
        i = 1 if sign > 0 else 0
        copy = pltpu.make_async_remote_copy(
            src_ref=relay.at[relays.index((k, g))],
            dst_ref=fields.at[k, g, 0 if sign > 0 else X + 1, 1 : Y + 1],
            send_sem=rsend.at[0], recv_sem=xrecv.at[k, g, i],
            device_id={"gx": 2 if sign > 0 else 1}, device_id_type=MESH)
        return copy

    ways = [(a, s) for a in AXES if count[a] > 1 for s in (-1, 1)]

    def inner(sign):
        return pos["gx"] == (1 if sign > 0 else 2)

    def send(k, g, axes, signs=(-1, 1), also=None):
        go = []
        for a, s in ways:
            if a in axes and s in signs:
                copy, out, _ = halo(k, g, a, s)
                if also is not None:
                    out = out & also
                if a == "gx" and via:
                    far = inner(s) if also is None else inner(s) & also
                    go.insert(0, (far, hop(k, g, s) if relayed(k, g) else copy))
                    out = out & jnp.logical_not(inner(s))
                go.append((out, copy))
        for out, copy in go:
            pl.when(out)(copy.start)

    def wait_x(k, g):
        for a, s in ways:
            if a == "gx":
                copy, _, come = halo(k, g, a, s)
                pl.when(come)(copy.wait_recv)

    def wait_yz(k, h):
        r = pl.ds(h * GH, GH)
        for a, s in ways:
            if a == "gx":
                continue
            i = AXES.index(a) * 2 + (s > 0)
            if a == "gy":
                d = fields.at[k, r, inner_rows if k == 0 else slice(1, X + 1), 0 if s > 0 else Y + 1]
            else:
                d = zin.at[k, r, 0 if s > 0 else 1]
            come = pos[a] > 0 if s > 0 else pos[a] < count[a] - 1
            pl.when(come)(pltpu.make_async_copy(d, d, yzrecv.at[k, h, i - 2]).wait)

    def forwards(k, g):
        if relayed(k, g):
            for s, at in ((1, 3), (-1, 0)):
                @pl.when(pos["gx"] == at)
                def _(s=s):
                    hop(k, g, s).wait_recv()
                    forward(k, g, s).start()

    def wait_sends():
        for a, s in ways:
            i = AXES.index(a) * 2 + (s > 0)
            if a == "gx":
                d = fields.at[:, :, X if s > 0 else 1, 1 : Y + 1]
            elif a == "gy":
                d = fields.at[:, :, 1 : X + 1, Y if s > 0 else 1]
            else:
                d = zout
            out = pos[a] < count[a] - 1 if s > 0 else pos[a] > 0
            pl.when(out)(pltpu.make_async_copy(d, d, hsend.at[i]).wait)
            if a == "gz":
                pl.when(out)(pltpu.make_async_copy(zout_e, zout_e, hsend.at[6 + (s > 0)]).wait)
        if relays:
            @pl.when((pos["gx"] == 0) | (pos["gx"] == 3))
            def _():
                pltpu.make_async_copy(relay, relay, rsend.at[0]).wait()

        def sent(i, n, buf):
            if n:
                r = buf.at[pl.ds(0, n)]
                pltpu.make_async_copy(r, r, send_sem.at[i]).wait()

        def owned():
            sent(0, NO - 1, part)
            sent(1, NZ - 1, got2)
            sent(2, PL - 1, got1)

        when(mine, owned)
        if OW > 1:
            when(jnp.logical_not(mine), lambda: sent(0, NO, part))

    def pack(k, g):
        out = zero
        for x in range(X):
            for y in range(Y):
                l = x * Y + y
                f = pltpu.roll(fields[k, g, x + 1, y + 1], (2 * l + 1) % Z, 1)
                out = jnp.where(pair == l, f, out)
        zout[k, g] = out

    def pack_edges(g):
        out = zero
        for x in (0, X - 1):
            for y in range(Y):
                l = x * Y + y
                f = pltpu.roll(fields[0, g, x + 1, y + 1], (2 * l + 1) % Z, 1)
                out = jnp.where(pair == l, f, out)
        zout_e[g] = out

    def first(x):
        corr = lax.dot_general(
            coef, eig_v[x], (((1,), (1,)), ((), ())), preferred_element_type=jnp.float32)
        for g in range(G):
            for y in range(Y):
                s = src[g, x, y] + corr[g * CG : (g + 1) * CG, y * Z : (y + 1) * Z]
                src[g, x, y] = s
                f = s * rdv[x, y : y + 1]
                fields[0, g, x + 1, y + 1] = f

    edges = (0, X - 1)
    up_first = pos["gx"] < (count["gx"] + 1) // 2
    xa = jnp.where(up_first, X - 1, 0)
    for x, turn in ((xa, up_first), (X - 1 - xa, jnp.logical_not(up_first))):
        first(x)
        for g in range(G):
            send(0, g, ("gx",), (1,), turn)
            send(0, g, ("gx",), (-1,), jnp.logical_not(turn))
    for g in range(G):
        pack_edges(g)
    send_early()
    for x in range(1, X - 1):
        first(x)
    for g in range(G):
        send(0, g, ("gy",))
    for g in range(G):
        pack(0, g)
        send(0, g, ("gz",))

    def step(k, g, x, comb):
        for y in range(Y):
            l = x * Y + y
            f = fields[k, g, x + 1, y + 1]
            t = fields[k, g, x + 2, y + 1] + fields[k, g, x, y + 1]
            t = t + (fields[k, g, x + 1, y + 2] + fields[k, g, x + 1, y])
            out = pltpu.roll(comb, (2 * Z - 2 * l - 2) % Z, 1)
            up = jnp.where(at_high, out, pltpu.roll(f, Z - 1, 1))
            down = jnp.where(at_low, out, pltpu.roll(f, 1, 1))
            v = (src[g, x, y] + (t + (up + down))) * rdv[x, y : y + 1]
            if k < S - 1:
                fields[k + 1, g, x + 1, y + 1] = v
            else:
                at = pl.ds(g * CG * PT + l, CG, stride=PT)
                out_v[at, :] = v + cur_v[at, :]

    pltpu.make_async_copy(cur_h, cur_v.at[pl.ds(0, C * XY)], load_sem.at[3]).wait()
    for k in range(S):
        held, done, ready = {}, [], []

        def begin(op, g, k=k, held=held, ready=ready):
            if op == "E" and k == 0:
                if "E" not in ready:
                    ready.append("E")
                    wait_early()
                return jnp.where(odd, zin_e[1, g], pltpu.roll(zin_e[0, g], 2, 1))
            if g // GH not in ready:
                ready.append(g // GH)
                wait_yz(k, g // GH)
            if g not in held:
                held[g] = jnp.where(odd, zin[k, g, 1], pltpu.roll(zin[k, g, 0], 2, 1))
            return held[g]

        for op, g in ((o[0], int(o[1:])) for o in ORDER[k]):
            if op == "F":
                forwards(k, g)
                continue
            comb = begin(op, g)
            if op == "E":
                wait_x(k, g)
            for x in edges if op == "E" else range(1, X - 1):
                step(k, g, x, comb)
            done.append(g)
            if k < S - 1:
                if op == "E":
                    send(k + 1, g, ("gx",))
                if done.count(g) == 2:
                    send(k + 1, g, ("gy",))
                    pack(k + 1, g)
                    send(k + 1, g, ("gz",))
    wait_sends()


def finish(v, out_h, sem):
    C, XY, _ = out_h.shape
    c = pltpu.make_async_copy(v.at[:, pl.ds(0, XY)], out_h, sem)
    c.start()
    c.wait()


def body(sizes, gradient, noise_draw, current, eigvectors, eigvalues, reaction):
    C, X, Y, Z = gradient.shape
    R = eigvectors.shape[3]
    NX, NY, NZ = sizes
    PL = NX * NY
    G = GROUPS
    CG = C // G
    S = SWEEPS - 1
    XY = X * Y
    PT = pitch_of(XY)
    f32, bf16 = jnp.float32, jnp.bfloat16
    NO = PL // 2 if NY % 2 == 0 else PL
    rows = C * R // 128 // NO
    NR = max(sum(len(r) for r in RELAYED), 1)
    any_space = pl.BlockSpec(memory_space=pltpu.HBM)
    vmem = pl.BlockSpec(memory_space=pltpu.VMEM)
    dma = pltpu.SemaphoreType.DMA
    held = pl.pallas_call(
        functools.partial(kernel, sizes, (C, X, Y, Z, R)),
        out_shape=pltpu.VMEM((C * PT, Z), f32),
        in_specs=[any_space] * 6,
        out_specs=vmem,
        scratch_shapes=[
            pltpu.VMEM((X, Y * Z, R), bf16),
            pltpu.VMEM((C * XY, Z), bf16),
            pltpu.VMEM((C * XY, Z), bf16),
            pltpu.VMEM((C * PT, Z), f32),
            pltpu.VMEM((C * PT, Z), f32),
            pltpu.VMEM((C * PT, Z), f32),
            pltpu.VMEM((1, R), f32),
            pltpu.VMEM((X, Y, Z), f32),
            pltpu.VMEM((G, X, Y, CG, Z), f32),
            pltpu.VMEM((S, G, X + 2, Y + 2, CG, Z), f32),
            pltpu.VMEM((S, G, CG, Z), f32),
            pltpu.VMEM((S, G, 2, CG, Z), f32),
            pltpu.VMEM((G, CG, Z), f32),
            pltpu.VMEM((2, G, CG, Z), f32),
            pltpu.VMEM((NR, Y, CG, Z), f32),
            pltpu.VMEM((NO, rows, 128), f32),
            pltpu.VMEM((PL, rows, 128), f32),
            pltpu.VMEM((NZ, rows, 128), f32),
            pltpu.VMEM((NO, rows, 128), f32),
            dma((5 + X,)),
            dma((3,)),
            dma((max(PL - 1, 1),)), dma((max(NZ - 1, 1),)), dma((max(PL - 1, 1),)),
            dma((8,)), dma((S, G, 2)), dma((S, HALVES, 4)), dma((4,)),
            dma((1,)), dma((NR,)),
        ],
        compiler_params=pltpu.CompilerParams(
            collective_id=0, has_side_effects=True, vmem_limit_bytes=67043328 - C * PT * Z * 4 - LEFT
        ),
    )(
        gradient.reshape(C * XY, Z),
        noise_draw.reshape(C * XY, Z),
        current.reshape(C * XY, Z),
        eigvectors.reshape(X, Y * Z, R),
        eigvalues.reshape(1, R),
        reaction,
    )
    out = pl.pallas_call(
        finish,
        out_shape=jax.ShapeDtypeStruct((C, XY, Z), f32),
        in_specs=[vmem],
        out_specs=any_space,
        scratch_shapes=[dma],
        compiler_params=pltpu.CompilerParams(vmem_limit_bytes=4 * 1024 * 1024),
    )(held.reshape(C, PT, Z))
    return out.reshape(current.shape)


def solution(mesh):
    return jax.shard_map(
        functools.partial(body, tuple(mesh.shape[a] for a in AXES)),
        mesh=mesh,
        in_specs=(
            P(None, "gx", "gy", "gz"),
            P(None, "gx", "gy", "gz"),
            P(None, "gx", "gy", "gz"),
            P("gx", "gy", "gz", None),
            P(),
            P("gx", "gy", "gz"),
        ),
        out_specs=P(None, "gx", "gy", "gz"),
        check_vma=False,
    )
```
